512 devices in a mesh: grp: 2 (over y), seq: 16 (over z), head: 8 (over x), sub: 2 (over core).
Axes of the slice: x: 8, y: 2, z: 16, core: 2. Of those that a mesh axis runs over, the one named last changes fastest.
The devices are a block of a 8x8x16 slice.
Arguments:
- vid_q: bfloat16 [10240, 4096], P(('grp', 'seq', 'sub'), 'head'), parts along dimension 0, may hold values from -6 to 6
- vid_k: bfloat16 [10240, 4096], P(('grp', 'seq', 'sub'), 'head'), parts along dimension 0, may hold values from -6 to 6
- vid_v: bfloat16 [10240, 4096], P(('grp', 'seq', 'sub'), 'head'), parts along dimension 0, may hold values from -6 to 6
- aud_q: bfloat16 [2560, 2048], P(('grp', 'seq', 'sub'), 'head'), parts along dimension 0, may hold values from -6 to 6
- cross_k: bfloat16 [10240, 2048], P(('grp', 'seq', 'sub'), 'head'), parts along dimension 0, may hold values from -6 to 6
- cross_v: bfloat16 [10240, 2048], P(('grp', 'seq', 'sub'), 'head'), parts along dimension 0, may hold values from -6 to 6
- cross_q: bfloat16 [10240, 2048], P(('grp', 'seq', 'sub'), 'head'), parts along dimension 0, may hold values from -6 to 6
- aud_k: bfloat16 [2560, 2048], P(('grp', 'seq', 'sub'), 'head'), parts along dimension 0, may hold values from -6 to 6
- aud_v: bfloat16 [2560, 2048], P(('grp', 'seq', 'sub'), 'head'), parts along dimension 0, may hold values from -6 to 6
- windows: int32 [2, 320], P(None, 'grp'), parts along dimension 1, may hold values from 0 to 160, as said below
Outputs:
- video_self: bfloat16 [10240, 4096], P(('grp', 'seq', 'sub'), 'head'), parts along dimension 0
- audio_out: bfloat16 [2560, 2048], P(('grp', 'seq', 'sub'), 'head'), parts along dimension 0
- video_cross: bfloat16 [10240, 2048], P(('grp', 'seq', 'sub'), 'head'), parts along dimension 0
The draws below stay inside these ranges and needn't reach their ends.
There are 2 independent parts, one for each index of `grp`. The reference program is written for one: setup_inputs(seed, part) draws one part's arguments, and reference() takes and returns one part's arrays. A program takes and returns all parts, laid end to end along the dimension named above; each array names one. Nothing has to cross between parts.
Inputs may be any that keep to these rules, and one draw needn't show every extreme that they name: For every stretch c, windows[0, c] lies between max(0, c - 5) and c, and windows[1, c] between c + 1 and min(160, c + 6); in every draw some stretch reaches 5 tiles on both sides.
All inputs are finite; a program needn't handle non-finite values.
Results may differ from the reference program's by a relative error of at most 0.03.
Values may be sent and summed in bfloat16 or wider, within the bound.
No kernel may reach another device: no remote copies, remote signals or barrier semaphores. Data moves between devices by JAX's collectives and lax.ppermute only.
A program may use at most 64 MiB of HBM per device.

```python
import jax
import jax.numpy as jnp
from jax import lax

VIDEO_HEADS = 32
HEAD_DIM = 128
AUDIO_HEADS = 32
AUDIO_DIM = 64
TILE_LEN = 32
STRETCH_LEN = 8
WINDOW_REACH = 5
VIDEO_TOKENS = 5120
AUDIO_TOKENS = 1280
TILE_COUNT = 160


def drawn(key, query_rows, key_rows, width):
    base_query = jnp.clip(jax.random.normal(jax.random.fold_in(key, 11), (query_rows, width), jnp.float32), -5.0, 5.0)
    base_key = jnp.clip(jax.random.normal(jax.random.fold_in(key, 12), (key_rows, width), jnp.float32), -5.0, 5.0)
    return (base_query, base_key)


def video_pair(key):
    return drawn(jax.random.fold_in(key, 1), VIDEO_TOKENS, VIDEO_TOKENS, VIDEO_HEADS * HEAD_DIM)


def audio_pair(key):
    return drawn(jax.random.fold_in(key, 2), AUDIO_TOKENS, VIDEO_TOKENS, AUDIO_HEADS * AUDIO_DIM)


def window_pair(key):
    return drawn(jax.random.fold_in(key, 3), VIDEO_TOKENS, AUDIO_TOKENS, AUDIO_HEADS * AUDIO_DIM)


def draw_vid_q(key, part):
    return video_pair(key)[0].astype(jnp.bfloat16)


def draw_vid_k(key, part):
    return video_pair(key)[1].astype(jnp.bfloat16)


def draw_aud_q(key, part):
    return audio_pair(key)[0].astype(jnp.bfloat16)


def draw_cross_k(key, part):
    return audio_pair(key)[1].astype(jnp.bfloat16)


def draw_cross_q(key, part):
    return window_pair(key)[0].astype(jnp.bfloat16)


def draw_aud_k(key, part):
    return window_pair(key)[1].astype(jnp.bfloat16)


def draw_windows(key, part):
    below = jax.random.randint(jax.random.fold_in(key, 41), (TILE_COUNT,), 0, WINDOW_REACH + 1)
    above = jax.random.randint(jax.random.fold_in(key, 42), (TILE_COUNT,), 0, WINDOW_REACH + 1)
    chosen = jax.random.randint(jax.random.fold_in(key, 43), (), WINDOW_REACH, TILE_COUNT - WINDOW_REACH)
    below = below.at[chosen].set(WINDOW_REACH)
    above = above.at[chosen].set(WINDOW_REACH)
    stretch_ids = jnp.arange(TILE_COUNT, dtype=jnp.int32)
    first_tile = jnp.maximum(stretch_ids - below, 0)
    after_tile = jnp.minimum(stretch_ids + 1 + above, TILE_COUNT)
    return jnp.stack([first_tile, after_tile]).astype(jnp.int32)


def levels(stream_key, extent, cuts, low, largest):
    loudness, own = 1.0, jax.random.fold_in(stream_key, 6)
    for dim, parts in cuts:
        heights = jnp.exp(jax.random.uniform(jax.random.fold_in(own, dim), (parts,), jnp.float32, low / len(cuts), largest / len(cuts)))
        loudness = loudness * jnp.repeat(heights, extent[dim] // parts).reshape([-1 if axis == dim else 1 for axis in range(len(extent))])
    return loudness


def normal_values(own_key, shape, deviation, limit, cuts=(), held_as=jnp.bfloat16):
    values = jax.random.normal(own_key, shape, jnp.float32) * deviation
    if len(cuts) > 0:
        values = levels(own_key, shape, cuts, -0.22, 0.18) * values
    return jnp.clip(values, min=-limit, max=limit).astype(held_as)


def setup_inputs(seed: int = 0, part: int = 0) -> dict:
    key_of = jax.random.split(jax.random.key(seed), 11)
    part_keys = jax.random.split(jax.random.fold_in(key_of[10], part), 11)
    return {
        "vid_q": draw_vid_q(jax.random.fold_in(jax.random.fold_in(key_of[10], part), 71), part),
        "vid_k": draw_vid_k(jax.random.fold_in(jax.random.fold_in(key_of[10], part), 71), part),
        "vid_v": normal_values(part_keys[2], (VIDEO_TOKENS, VIDEO_HEADS * HEAD_DIM), 1.0, 6.0, ((0, 32), (1, 8))),
        "aud_q": draw_aud_q(jax.random.fold_in(jax.random.fold_in(key_of[10], part), 71), part),
        "cross_k": draw_cross_k(jax.random.fold_in(jax.random.fold_in(key_of[10], part), 71), part),
        "cross_v": normal_values(part_keys[5], (VIDEO_TOKENS, AUDIO_HEADS * AUDIO_DIM), 1.0, 6.0, ((0, 32), (1, 8))),
        "cross_q": draw_cross_q(jax.random.fold_in(jax.random.fold_in(key_of[10], part), 71), part),
        "aud_k": draw_aud_k(jax.random.fold_in(jax.random.fold_in(key_of[10], part), 71), part),
        "aud_v": normal_values(part_keys[8], (AUDIO_TOKENS, AUDIO_HEADS * AUDIO_DIM), 1.0, 6.0, ((0, 32), (1, 8))),
        "windows": draw_windows(jax.random.fold_in(jax.random.fold_in(key_of[10], part), 71), part),
    }


def attend(queries, key_rows, value_rows, scaling, visible):
    scores = jnp.dot(queries, key_rows.T, preferred_element_type=jnp.float32) * scaling
    scores = jnp.where(visible, scores, jnp.float32(-1e30))
    peak = jnp.max(scores, axis=1, keepdims=True)
    weights = jnp.exp(scores - peak)
    summed = jnp.sum(weights, axis=1, keepdims=True)
    mixed = jnp.dot(weights.astype(jnp.bfloat16), value_rows, preferred_element_type=jnp.float32)
    return mixed / summed


def split_heads(matrix, head_count):
    return matrix.reshape(matrix.shape[0], head_count, -1).transpose(1, 0, 2)


def multi_head(queries, key_rows, value_rows, head_count, head_size, visible):
    scaling = 1.0 / (head_size ** 0.5)

    def one_head(triple):
        return attend(triple[0], triple[1], triple[2], scaling, visible)

    stacked = lax.map(one_head, (split_heads(queries, head_count), split_heads(key_rows, head_count), split_heads(value_rows, head_count)))
    return stacked.transpose(1, 0, 2).reshape(queries.shape[0], -1).astype(jnp.bfloat16)


def reference(vid_q, vid_k, vid_v, aud_q, cross_k, cross_v, cross_q, aud_k, aud_v, windows):
    video_self = multi_head(vid_q, vid_k, vid_v, VIDEO_HEADS, HEAD_DIM, True)
    audio_out = multi_head(aud_q, cross_k, cross_v, AUDIO_HEADS, AUDIO_DIM, True)
    video_tile = jnp.arange(VIDEO_TOKENS, dtype=jnp.int32) // TILE_LEN
    audio_stretch = jnp.arange(AUDIO_TOKENS, dtype=jnp.int32) // STRETCH_LEN
    first_tile = windows[0][audio_stretch]
    after_tile = windows[1][audio_stretch]
    visible = (first_tile[None, :] <= video_tile[:, None]) & (video_tile[:, None] < after_tile[None, :])
    video_cross = multi_head(cross_q, aud_k, aud_v, AUDIO_HEADS, AUDIO_DIM, visible)
    return video_self, audio_out, video_cross
```

```python
import math

import jax
import jax.numpy as jnp
from jax import lax
from jax.experimental import pallas as pl
from jax.experimental.pallas import tpu as pltpu
from jax.sharding import PartitionSpec as P

HEAD_DIM = 128
AUDIO_DIM = 64
TILE_LEN = 32
STRETCH_LEN = 8
LANES = 128
LOG2E = math.log2(math.e)
STOPS = 4


def dot_t(a, b):
    return lax.dot_general(a, b, (((1,), (1,)), ((), ())), preferred_element_type=jnp.float32)


def dot_n(a, b):
    return lax.dot_general(a, b, (((1,), (0,)), ((), ())), preferred_element_type=jnp.float32)


def joined(parts):
    return parts[0] if len(parts) == 1 else jnp.concatenate(parts, axis=0)


def kernel_call(kernel, out_shape, cost, *operands):
    return pl.pallas_call(
        kernel,
        out_shape=out_shape,
        cost_estimate=pl.CostEstimate(flops=cost, transcendentals=0, bytes_accessed=0),
        compiler_params=pltpu.CompilerParams(vmem_limit_bytes=48 * 1024 * 1024),
    )(*operands)


def video_fold(queries, pairs, states):
    sets, rows, width = (len(queries), queries[0].shape[0], queries[0].shape[1])
    heads = width // HEAD_DIM
    factor = LOG2E / math.sqrt(HEAD_DIM)
    count = len(pairs)

    def kernel(*refs):
        q_refs, refs = (refs[:sets], refs[sets:])
        k_refs, v_refs, refs = (refs[:count], refs[count : 2 * count], refs[2 * count :])
        s_refs, o_refs = (refs[:-sets], refs[-sets:])
        lane = lax.broadcasted_iota(jnp.int32, (rows, LANES), 1)
        tails = [jnp.zeros((rows, LANES), jnp.float32) for _ in range(sets)]
        for h in range(heads):
            cols = slice(h * HEAD_DIM, (h + 1) * HEAD_DIM)
            keys = joined([r[:, cols] for r in k_refs])
            values = joined([r[:, cols] for r in v_refs])
            for i in range(sets):
                scores = dot_t(q_refs[i][:, cols], keys)
                newest = jnp.max(scores, axis=1, keepdims=True)
                if s_refs:
                    before = s_refs[i][:, width + h : width + h + 1]
                    newest = jnp.maximum(newest, before)
                weights = jnp.exp2((scores - newest) * factor)
                summed = jnp.sum(weights, axis=1, keepdims=True)
                mixed = dot_n(weights.astype(jnp.bfloat16), values)
                if s_refs:
                    shrink = jnp.exp2((before - newest) * factor)
                    summed = summed + shrink * s_refs[i][:, width + heads + h : width + heads + h + 1]
                    mixed = mixed + shrink * s_refs[i][:, cols]
                o_refs[i][:, cols] = mixed
                tails[i] = jnp.where(lane == h, newest, jnp.where(lane == heads + h, summed, tails[i]))
        for i in range(sets):
            o_refs[i][:, width:] = tails[i]

    keys_total = sum(k.shape[0] for k, _ in pairs)
    return kernel_call(
        kernel,
        [jax.ShapeDtypeStruct((rows, width + LANES), jnp.float32)] * sets,
        4 * sets * rows * keys_total * width,
        *queries,
        *[k for k, _ in pairs],
        *[v for _, v in pairs],
        *states,
    )


def video_finish(own, other):
    rows, width = (own.shape[0], own.shape[1] - LANES)
    heads = width // HEAD_DIM
    factor = LOG2E / math.sqrt(HEAD_DIM)

    def kernel(a_ref, b_ref, o_ref):
        for h in range(heads):
            cols = slice(h * HEAD_DIM, (h + 1) * HEAD_DIM)
            am, bm = (r[:, width + h : width + h + 1] for r in (a_ref, b_ref))
            al, bl = (r[:, width + heads + h : width + heads + h + 1] for r in (a_ref, b_ref))
            newest = jnp.maximum(am, bm)
            aw, bw = (jnp.exp2((am - newest) * factor), jnp.exp2((bm - newest) * factor))
            scale = 1.0 / (aw * al + bw * bl)
            mixed = a_ref[:, cols] * (aw * scale) + b_ref[:, cols] * (bw * scale)
            o_ref[:, cols] = mixed.astype(jnp.bfloat16)

    return kernel_call(
        kernel, jax.ShapeDtypeStruct((rows, width), jnp.bfloat16), rows * width * 8, own, other
    )


def one_head(pair, parity):
    lane = lax.broadcasted_iota(jnp.int32, pair.shape, 1)
    keep = (lane < AUDIO_DIM) if parity == 0 else (lane >= AUDIO_DIM)
    return jnp.where(keep, pair, jnp.zeros_like(pair))


def audio_part(queries, blocks, places):
    total, width = queries.shape
    rows = total // places
    heads = width // AUDIO_DIM
    factor = LOG2E / math.sqrt(AUDIO_DIM)
    taken = blocks[0].shape[0]
    count = len(blocks)

    def kernel(q_ref, *refs):
        b_refs, o_refs = (refs[:count], refs[count:])
        lane = lax.broadcasted_iota(jnp.int32, (total, LANES), 1)
        tail = jnp.zeros((total, LANES), jnp.float32)
        for g in range(heads // 2):
            cols = slice(g * LANES, (g + 1) * LANES)
            keys = joined([r[:taken, cols] for r in b_refs])
            values = joined([r[:taken, width + g * LANES : width + (g + 1) * LANES] for r in b_refs])
            pair = q_ref[:, cols]
            mixed = []
            for parity in range(2):
                h = 2 * g + parity
                scores = dot_t(one_head(pair, parity), keys)
                newest = jnp.max(scores, axis=1, keepdims=True)
                weights = jnp.exp2((scores - newest) * factor)
                summed = jnp.sum(weights, axis=1, keepdims=True)
                mixed.append(dot_n(weights.astype(jnp.bfloat16), values) / summed)
                level = newest * factor + jnp.log2(summed)
                high = level.astype(jnp.bfloat16).astype(jnp.float32)
                middle = (level - high).astype(jnp.bfloat16).astype(jnp.float32)
                low = level - high - middle
                for j, part in enumerate((high, middle, low)):
                    tail = jnp.where(lane == j * heads + h, part, tail)
            both = jnp.where(lane < AUDIO_DIM, mixed[0], mixed[1])
            for i in range(places):
                o_refs[i][:, cols] = both[i * rows : (i + 1) * rows].astype(jnp.bfloat16)
        for i in range(places):
            o_refs[i][:, width:] = tail[i * rows : (i + 1) * rows].astype(jnp.bfloat16)

    return kernel_call(
        kernel,
        [jax.ShapeDtypeStruct((rows, width + LANES), jnp.bfloat16)] * places,
        4 * total * taken * count * width,
        queries,
        *blocks,
    )


def audio_finish(parts):
    rows, width = (parts[0].shape[0], parts[0].shape[1] - LANES)
    heads = width // AUDIO_DIM

    def kernel(*refs):
        p_refs, o_ref = (refs[:-1], refs[-1])
        tails = [r[:, width:].astype(jnp.float32) for r in p_refs]
        shares = []
        for h in range(heads):
            levels = [sum(t[:, j * heads + h : j * heads + h + 1] for j in range(3)) for t in tails]
            newest = levels[0]
            for level in levels[1:]:
                newest = jnp.maximum(newest, level)
            powers = [jnp.exp2(level - newest) for level in levels]
            scale = 1.0 / sum(powers)
            shares.append([p * scale for p in powers])
        lane = lax.broadcasted_iota(jnp.int32, (rows, LANES), 1)
        for g in range(heads // 2):
            cols = slice(g * LANES, (g + 1) * LANES)
            mixed = jnp.zeros((rows, LANES), jnp.float32)
            for i, r in enumerate(p_refs):
                share = jnp.where(lane < AUDIO_DIM, shares[2 * g][i], shares[2 * g + 1][i])
                mixed = mixed + share * r[:, cols].astype(jnp.float32)
            o_ref[:, cols] = mixed.astype(jnp.bfloat16)

    return kernel_call(
        kernel, jax.ShapeDtypeStruct((rows, width), jnp.bfloat16), rows * width * 16, *parts
    )


def window_attend(queries, near, offsets, limits):
    rows, width = queries.shape
    heads = width // AUDIO_DIM
    factor = LOG2E / math.sqrt(AUDIO_DIM)
    span = limits.shape[1] // len(near)
    count = len(near)

    def kernel(q_ref, lim_ref, *refs):
        n_refs, o_ref = (refs[:count], refs[count])
        tile = lax.broadcasted_iota(jnp.int32, (rows, span), 0) // TILE_LEN
        visible = []
        for i in range(count):
            cut = slice(i * span, (i + 1) * span)
            visible.append((lim_ref[0:1, cut] <= tile) & (tile < lim_ref[1:2, cut]))
        lane = lax.broadcasted_iota(jnp.int32, (rows, LANES), 1)
        for g in range(heads // 2):
            cols = slice(g * LANES, (g + 1) * LANES)
            pair = q_ref[:, cols]
            mixed = []
            for parity in range(2):
                masked = one_head(pair, parity)
                scores = []
                for i in range(count):
                    keys = n_refs[i][offsets[i] : offsets[i] + span, cols]
                    scores.append(jnp.where(visible[i], dot_t(masked, keys), jnp.float32(-1e30)))
                newest = jnp.max(scores[0], axis=1, keepdims=True)
                for score in scores[1:]:
                    newest = jnp.maximum(newest, jnp.max(score, axis=1, keepdims=True))
                summed = jnp.zeros((rows, 1), jnp.float32)
                top = jnp.zeros((rows, LANES), jnp.float32)
                for i in range(count):
                    values = n_refs[i][
                        offsets[i] : offsets[i] + span, width + g * LANES : width + (g + 1) * LANES
                    ]
                    weights = jnp.exp2((scores[i] - newest) * factor)
                    summed = summed + jnp.sum(weights, axis=1, keepdims=True)
                    top = top + dot_n(weights.astype(jnp.bfloat16), values)
                mixed.append(top / summed)
            both = jnp.where(lane < AUDIO_DIM, mixed[0], mixed[1])
            o_ref[:, cols] = both.astype(jnp.bfloat16)

    return kernel_call(
        kernel,
        jax.ShapeDtypeStruct((rows, width), jnp.bfloat16),
        4 * rows * span * count * width,
        queries,
        limits,
        *near,
    )


def body(vid_q, vid_k, vid_v, aud_q, cross_k, cross_v, cross_q, aud_k, aud_v, windows):
    n = lax.axis_size("seq")
    if n % (2 * STOPS) != 0 or lax.axis_size("sub") != 2:
        raise ValueError("mesh shape")
    ring = []
    for z in range(n):
        ring.append((2 * z, 2 * ((z + 1) % n)))
        ring.append((2 * z + 1, 2 * ((z - 1) % n) + 1))

    def onward(array):
        return lax.ppermute(array, ("seq", "sub"), ring)

    def swap(array):
        return lax.ppermute(array, "sub", [(0, 1), (1, 0)])

    def shift(array, by):
        return lax.ppermute(array, "seq", [(z, (z + by) % n) for z in range(n)])

    passing = {("k", 0): vid_k, ("v", 0): vid_v}
    first_k = onward(vid_k)
    first_v = onward(vid_v)
    video_rows = cross_k.shape[0]
    audio_rows = aud_k.shape[0]
    near_own = jnp.concatenate((cross_k, cross_v), axis=1)
    audio_own = jnp.concatenate((aud_k, aud_v), axis=1)
    bundle = jnp.concatenate((near_own, audio_own), axis=0)
    other_k, other_v, other_q, other_bundle = (swap(vid_k), swap(vid_v), swap(vid_q), swap(bundle))

    step = n // STOPS
    hops = [step, -step, 2 * step]
    visitors = [shift(aud_q, by) for by in hops]
    near_one = onward(near_own)
    bundle_one = onward(other_bundle)
    bundle_two = onward(bundle_one)

    a_k, a_v = (first_k, first_v)
    b_k, b_v = (onward(other_k), onward(other_v))
    arrived = [[(vid_k, vid_v)], [(a_k, a_v), (b_k, b_v)]]
    for t in range(2, n // 2 + 1):
        a_k, a_v = (onward(a_k), onward(a_v))
        if t == n // 2:
            arrived.append([(a_k, a_v)])
            break
        b_k, b_v = (onward(b_k), onward(b_v))
        arrived.append([(a_k, a_v), (b_k, b_v)])

    audio_blocks = [near_own, other_bundle, near_one, bundle_one, bundle_two]
    audio_blocks += [swap(near_one), swap(bundle_one), swap(bundle_two)]
    pieces = audio_part(jnp.concatenate([aud_q] + visitors, axis=0), audio_blocks, STOPS)
    returned = [pieces[0]] + [shift(piece, -by) for piece, by in zip(pieces[1:], hops)]
    audio_out = audio_finish(returned)

    position = lax.axis_index(("seq", "sub"))
    stretches = audio_rows // STRETCH_LEN
    tiles = video_rows // TILE_LEN
    side = 2 * lax.axis_index("sub") - 1
    padded = jnp.pad(windows, ((0, 0), (stretches, stretches)))
    limits = jnp.concatenate(
        [
            lax.dynamic_slice_in_dim(padded, (position + d + 1) * stretches, stretches, axis=1)
            for d in (0, side, -side)
        ],
        axis=1,
    )
    limits = jnp.repeat(limits - position * tiles, STRETCH_LEN, axis=1)
    video_cross = window_attend(
        cross_q,
        [audio_own, bundle_one, other_bundle],
        [0, video_rows, video_rows],
        limits,
    )

    queries = [vid_q, other_q]
    states = video_fold(queries, arrived[0] + arrived[1], [])
    middle = arrived[2:-1]
    for i in range(0, len(middle), 2):
        pairs = [pair for group in middle[i : i + 2] for pair in group]
        states = video_fold(queries, pairs, states)
    away = video_fold(queries[1:], arrived[-1], states[1:])[0]
    home = video_fold(queries[:1], arrived[-1], states[:1])[0]
    video_self = video_finish(home, swap(away))
    return (video_self, audio_out, video_cross)


def solution(mesh):
    rows = P(("grp", "seq", "sub"), "head")
    return jax.shard_map(
        body,
        mesh=mesh,
        in_specs=(rows,) * 9 + (P(None, "grp"),),
        out_specs=(rows, rows, rows),
        check_vma=False,
    )
```

```python
import math

import jax
import jax.numpy as jnp
from jax import lax
from jax.experimental import pallas as pl
from jax.experimental.pallas import tpu as pltpu
from jax.sharding import PartitionSpec as P

HEAD_DIM = 128
AUDIO_DIM = 64
TILE_LEN = 32
STRETCH_LEN = 8
LANES = 128
LOG2E = math.log2(math.e)
STOPS = 4
VIDEO_BLOCKS = 8


def dot_t(a, b):
    return lax.dot_general(a, b, (((1,), (1,)), ((), ())), preferred_element_type=jnp.float32)


def dot_n(a, b):
    return lax.dot_general(a, b, (((1,), (0,)), ((), ())), preferred_element_type=jnp.float32)


def joined(parts):
    return parts[0] if len(parts) == 1 else jnp.concatenate(parts, axis=0)


def kernel_call(kernel, out_shape, cost, *operands):
    return pl.pallas_call(
        kernel,
        out_shape=out_shape,
        cost_estimate=pl.CostEstimate(flops=cost, transcendentals=0, bytes_accessed=0),
        compiler_params=pltpu.CompilerParams(vmem_limit_bytes=48 * 1024 * 1024),
    )(*operands)


def video_attend(queries, gathered):
    rows, width = queries.shape
    heads = width // HEAD_DIM
    factor = LOG2E / math.sqrt(HEAD_DIM)
    total = gathered.shape[0]
    block = total // VIDEO_BLOCKS

    def kernel(q_ref, k_ref, v_ref, o_ref, m_ref, l_ref, a_ref):
        step = pl.program_id(0)

        @pl.when(step == 0)
        def _():
            m_ref[...] = jnp.full(m_ref.shape, -jnp.inf, jnp.float32)
            l_ref[...] = jnp.zeros(l_ref.shape, jnp.float32)
            a_ref[...] = jnp.zeros(a_ref.shape, jnp.float32)

        for h in range(heads):
            cols = slice(h * HEAD_DIM, (h + 1) * HEAD_DIM)
            scores = dot_t(q_ref[:, cols], k_ref[:, cols])
            before = m_ref[h]
            newest = jnp.maximum(before, jnp.max(scores, axis=1, keepdims=True))
            weights = jnp.exp2((scores - newest[:, :1]) * factor)
            shrink = jnp.exp2((before - newest) * factor)
            parts = weights[:, :LANES]
            for j in range(1, block // LANES):
                parts = parts + weights[:, j * LANES : (j + 1) * LANES]
            l_ref[h] = l_ref[h] * shrink + parts
            mixed = dot_n(weights.astype(jnp.bfloat16), v_ref[:, cols])
            a_ref[:, cols] = a_ref[:, cols] * shrink + mixed
            m_ref[h] = newest

        @pl.when(step == VIDEO_BLOCKS - 1)
        def _():
            for h in range(heads):
                cols = slice(h * HEAD_DIM, (h + 1) * HEAD_DIM)
                summed = jnp.sum(l_ref[h], axis=1, keepdims=True)
                o_ref[:, cols] = (a_ref[:, cols] / summed).astype(jnp.bfloat16)

    return pl.pallas_call(
        kernel,
        grid=(VIDEO_BLOCKS,),
        in_specs=[
            pl.BlockSpec((rows, width), lambda i: (0, 0)),
            pl.BlockSpec((block, width), lambda i: (i, 0)),
            pl.BlockSpec((block, width), lambda i: (i, 1)),
        ],
        out_specs=pl.BlockSpec((rows, width), lambda i: (0, 0)),
        out_shape=jax.ShapeDtypeStruct((rows, width), jnp.bfloat16),
        scratch_shapes=[
            pltpu.VMEM((heads, rows, LANES), jnp.float32),
            pltpu.VMEM((heads, rows, LANES), jnp.float32),
            pltpu.VMEM((rows, width), jnp.float32),
        ],
        cost_estimate=pl.CostEstimate(
            flops=4 * rows * total * width, transcendentals=0, bytes_accessed=0
        ),
        compiler_params=pltpu.CompilerParams(vmem_limit_bytes=48 * 1024 * 1024),
    )(queries, gathered, gathered)


def one_head(pair, parity):
    lane = lax.broadcasted_iota(jnp.int32, pair.shape, 1)
    keep = (lane < AUDIO_DIM) if parity == 0 else (lane >= AUDIO_DIM)
    return jnp.where(keep, pair, jnp.zeros_like(pair))


def audio_part(queries, blocks, places):
    total, width = queries.shape
    rows = total // places
    heads = width // AUDIO_DIM
    factor = LOG2E / math.sqrt(AUDIO_DIM)
    taken = blocks[0].shape[0]
    count = len(blocks)

    def kernel(q_ref, *refs):
        b_refs, o_refs = (refs[:count], refs[count:])
        lane = lax.broadcasted_iota(jnp.int32, (total, LANES), 1)
        tail = jnp.zeros((total, LANES), jnp.float32)
        for g in range(heads // 2):
            cols = slice(g * LANES, (g + 1) * LANES)
            keys = joined([r[:taken, cols] for r in b_refs])
            values = joined([r[:taken, width + g * LANES : width + (g + 1) * LANES] for r in b_refs])
            pair = q_ref[:, cols]
            mixed = []
            for parity in range(2):
                h = 2 * g + parity
                scores = dot_t(one_head(pair, parity), keys)
                newest = jnp.max(scores, axis=1, keepdims=True)
                weights = jnp.exp2((scores - newest) * factor)
                summed = jnp.sum(weights, axis=1, keepdims=True)
                mixed.append(dot_n(weights.astype(jnp.bfloat16), values) / summed)
                level = newest * factor + jnp.log2(summed)
                high = level.astype(jnp.bfloat16).astype(jnp.float32)
                middle = (level - high).astype(jnp.bfloat16).astype(jnp.float32)
                low = level - high - middle
                for j, part in enumerate((high, middle, low)):
                    tail = jnp.where(lane == j * heads + h, part, tail)
            both = jnp.where(lane < AUDIO_DIM, mixed[0], mixed[1])
            for i in range(places):
                o_refs[i][:, cols] = both[i * rows : (i + 1) * rows].astype(jnp.bfloat16)
        for i in range(places):
            o_refs[i][:, width:] = tail[i * rows : (i + 1) * rows].astype(jnp.bfloat16)

    return kernel_call(
        kernel,
        [jax.ShapeDtypeStruct((rows, width + LANES), jnp.bfloat16)] * places,
        4 * total * taken * count * width,
        queries,
        *blocks,
    )


def audio_finish(parts):
    rows, width = (parts[0].shape[0], parts[0].shape[1] - LANES)
    heads = width // AUDIO_DIM

    def kernel(*refs):
        p_refs, o_ref = (refs[:-1], refs[-1])
        tails = [r[:, width:].astype(jnp.float32) for r in p_refs]
        shares = []
        for h in range(heads):
            levels = [sum(t[:, j * heads + h : j * heads + h + 1] for j in range(3)) for t in tails]
            newest = levels[0]
            for level in levels[1:]:
                newest = jnp.maximum(newest, level)
            powers = [jnp.exp2(level - newest) for level in levels]
            scale = 1.0 / sum(powers)
            shares.append([p * scale for p in powers])
        lane = lax.broadcasted_iota(jnp.int32, (rows, LANES), 1)
        for g in range(heads // 2):
            cols = slice(g * LANES, (g + 1) * LANES)
            mixed = jnp.zeros((rows, LANES), jnp.float32)
            for i, r in enumerate(p_refs):
                share = jnp.where(lane < AUDIO_DIM, shares[2 * g][i], shares[2 * g + 1][i])
                mixed = mixed + share * r[:, cols].astype(jnp.float32)
            o_ref[:, cols] = mixed.astype(jnp.bfloat16)

    return kernel_call(
        kernel, jax.ShapeDtypeStruct((rows, width), jnp.bfloat16), rows * width * 16, *parts
    )


def window_attend(queries, near, offsets, limits):
    rows, width = queries.shape
    heads = width // AUDIO_DIM
    factor = LOG2E / math.sqrt(AUDIO_DIM)
    span = limits.shape[1] // len(near)
    count = len(near)

    def kernel(q_ref, lim_ref, *refs):
        n_refs, o_ref = (refs[:count], refs[count])
        tile = lax.broadcasted_iota(jnp.int32, (rows, span), 0) // TILE_LEN
        visible = []
        for i in range(count):
            cut = slice(i * span, (i + 1) * span)
            visible.append((lim_ref[0:1, cut] <= tile) & (tile < lim_ref[1:2, cut]))
        lane = lax.broadcasted_iota(jnp.int32, (rows, LANES), 1)
        for g in range(heads // 2):
            cols = slice(g * LANES, (g + 1) * LANES)
            pair = q_ref[:, cols]
            mixed = []
            for parity in range(2):
                masked = one_head(pair, parity)
                scores = []
                for i in range(count):
                    keys = n_refs[i][offsets[i] : offsets[i] + span, cols]
                    scores.append(jnp.where(visible[i], dot_t(masked, keys), jnp.float32(-1e30)))
                newest = jnp.max(scores[0], axis=1, keepdims=True)
                for score in scores[1:]:
                    newest = jnp.maximum(newest, jnp.max(score, axis=1, keepdims=True))
                summed = jnp.zeros((rows, 1), jnp.float32)
                top = jnp.zeros((rows, LANES), jnp.float32)
                for i in range(count):
                    values = n_refs[i][
                        offsets[i] : offsets[i] + span, width + g * LANES : width + (g + 1) * LANES
                    ]
                    weights = jnp.exp2((scores[i] - newest) * factor)
                    summed = summed + jnp.sum(weights, axis=1, keepdims=True)
                    top = top + dot_n(weights.astype(jnp.bfloat16), values)
                mixed.append(top / summed)
            both = jnp.where(lane < AUDIO_DIM, mixed[0], mixed[1])
            o_ref[:, cols] = both.astype(jnp.bfloat16)

    return kernel_call(
        kernel,
        jax.ShapeDtypeStruct((rows, width), jnp.bfloat16),
        4 * rows * span * count * width,
        queries,
        limits,
        *near,
    )


def body(vid_q, vid_k, vid_v, aud_q, cross_k, cross_v, cross_q, aud_k, aud_v, windows):
    n = lax.axis_size("seq")
    if n % (2 * STOPS) != 0 or lax.axis_size("sub") != 2:
        raise ValueError("mesh shape")
    ring = []
    for z in range(n):
        ring.append((2 * z, 2 * ((z + 1) % n)))
        ring.append((2 * z + 1, 2 * ((z - 1) % n) + 1))

    def onward(array):
        return lax.ppermute(array, ("seq", "sub"), ring)

    def swap(array):
        return lax.ppermute(array, "sub", [(0, 1), (1, 0)])

    def shift(array, by):
        return lax.ppermute(array, "seq", [(z, (z + by) % n) for z in range(n)])

    video_rows = cross_k.shape[0]
    audio_rows = aud_k.shape[0]
    gathered = lax.all_gather(
        jnp.concatenate((vid_k, vid_v), axis=1), ("seq", "sub"), axis=0, tiled=True
    )
    near_own = jnp.concatenate((cross_k, cross_v), axis=1)
    audio_own = jnp.concatenate((aud_k, aud_v), axis=1)
    bundle = jnp.concatenate((near_own, audio_own), axis=0)
    other_bundle = swap(bundle)

    step = n // STOPS
    hops = [step, -step, 2 * step]
    visitors = [shift(aud_q, by) for by in hops]
    near_one = onward(near_own)
    bundle_one = onward(other_bundle)
    bundle_two = onward(bundle_one)

    audio_blocks = [near_own, other_bundle, near_one, bundle_one, bundle_two]
    audio_blocks += [swap(near_one), swap(bundle_one), swap(bundle_two)]
    pieces = audio_part(jnp.concatenate([aud_q] + visitors, axis=0), audio_blocks, STOPS)
    returned = [pieces[0]] + [shift(piece, -by) for piece, by in zip(pieces[1:], hops)]
    audio_out = audio_finish(returned)

    position = lax.axis_index(("seq", "sub"))
    stretches = audio_rows // STRETCH_LEN
    tiles = video_rows // TILE_LEN
    side = 2 * lax.axis_index("sub") - 1
    padded = jnp.pad(windows, ((0, 0), (stretches, stretches)))
    limits = jnp.concatenate(
        [
            lax.dynamic_slice_in_dim(padded, (position + d + 1) * stretches, stretches, axis=1)
            for d in (0, side, -side)
        ],
        axis=1,
    )
    limits = jnp.repeat(limits - position * tiles, STRETCH_LEN, axis=1)
    video_cross = window_attend(
        cross_q,
        [audio_own, bundle_one, other_bundle],
        [0, video_rows, video_rows],
        limits,
    )

    video_self = video_attend(vid_q, gathered)
    return (video_self, audio_out, video_cross)


def solution(mesh):
    rows = P(("grp", "seq", "sub"), "head")
    return jax.shard_map(
        body,
        mesh=mesh,
        in_specs=(rows,) * 9 + (P(None, "grp"),),
        out_specs=(rows, rows, rows),
        check_vma=False,
    )
```

```python
import math

import jax
import jax.numpy as jnp
from jax import lax
from jax.experimental import pallas as pl
from jax.experimental.pallas import tpu as pltpu
from jax.sharding import PartitionSpec as P

HEAD_DIM = 128
AUDIO_DIM = 64
TILE_LEN = 32
STRETCH_LEN = 8
LANES = 128
LOG2E = math.log2(math.e)
VIDEO_FACTOR = LOG2E / math.sqrt(HEAD_DIM)
AUDIO_FACTOR = LOG2E / math.sqrt(AUDIO_DIM)


def dot_t(a, b):
    return lax.dot_general(a, b, (((1,), (1,)), ((), ())), preferred_element_type=jnp.float32)


def dot_n(a, b):
    return lax.dot_general(a, b, (((1,), (0,)), ((), ())), preferred_element_type=jnp.float32)


def lane_of(rows):
    return lax.broadcasted_iota(jnp.int32, (rows, LANES), 1)


def kernel_call(kernel, out_shape, cost, *operands, scalars=0, scratch=()):
    smem = pl.BlockSpec(memory_space=pltpu.SMEM)
    vmem = pl.BlockSpec(memory_space=pltpu.VMEM)
    return pl.pallas_call(
        kernel,
        in_specs=[smem] * scalars + [vmem] * (len(operands) - scalars),
        out_shape=out_shape,
        scratch_shapes=list(scratch),
        cost_estimate=pl.CostEstimate(flops=cost, transcendentals=0, bytes_accessed=0),
        compiler_params=pltpu.CompilerParams(vmem_limit_bytes=48 * 1024 * 1024),
    )(*operands)


def padded(rows):
    return -(-rows // 16) * 16


def pack_heads(arc, vid_q, vid_k, vid_v, aud_q, cross_k, cross_v):
    rows, width = vid_q.shape
    heads = width // HEAD_DIM
    visits = aud_q.shape[0]
    room = padded(visits)
    total = 4 * rows + room

    def kernel(arc_ref, q_ref, k_ref, v_ref, aq_ref, ck_ref, cv_ref, *refs):
        o_refs, held = (refs[:-1], refs[-1])
        for g in range(heads // 2):
            cols = slice(g * LANES, (g + 1) * LANES)
            aq, ck, cv = (r[:, cols].astype(jnp.float32) for r in (aq_ref, ck_ref, cv_ref))
            for parity in range(2):
                h = 2 * g + parity
                a, b, c = (aq, ck, cv)
                if parity == 0:
                    c = pltpu.roll(c, AUDIO_DIM, 1)
                else:
                    a, b = (pltpu.roll(a, AUDIO_DIM, 1), pltpu.roll(b, AUDIO_DIM, 1))
                a = jnp.where(lane_of(visits) < AUDIO_DIM, a, 0.0)
                a = jnp.concatenate((a, jnp.zeros((room - visits, LANES), jnp.float32)), axis=0)
                both = jnp.where(lane_of(rows) < AUDIO_DIM, b, c)
                wide = slice(h * LANES, (h + 1) * LANES)
                held[h, 0:rows] = q_ref[:, wide]
                held[h, rows : rows + room] = a.astype(jnp.bfloat16)
                held[h, rows + room : 2 * rows + room] = k_ref[:, wide]
                held[h, 2 * rows + room : 3 * rows + room] = v_ref[:, wide]
                held[h, 3 * rows + room :] = both.astype(jnp.bfloat16)
        for i in range(heads):
            o_refs[i][...] = held[lax.rem(arc_ref[0] + i, heads)]

    return kernel_call(
        kernel,
        [jax.ShapeDtypeStruct((total, LANES), jnp.bfloat16)] * heads,
        total * LANES * 64,
        arc,
        vid_q,
        vid_k,
        vid_v,
        aud_q,
        cross_k,
        cross_v,
        scalars=1,
        scratch=[pltpu.VMEM((heads, total, LANES), jnp.bfloat16)],
    )


def regroup(blocks, rows, room):
    places = len(blocks)

    def kernel(*refs):
        b_refs, q_ref, kv_ref = (refs[:places], refs[places], refs[places + 1])
        for i in range(places):
            q_ref[i * rows : (i + 1) * rows] = b_refs[i][0:rows]
            start = places * rows + i * room
            q_ref[start : start + room] = b_refs[i][rows : rows + room]
            for j in range(3):
                start = rows + room + j * rows
                kv_ref[(j * places + i) * rows : (j * places + i + 1) * rows] = b_refs[i][
                    start : start + rows
                ]

    return kernel_call(
        kernel,
        [
            jax.ShapeDtypeStruct((places * (rows + room), LANES), jnp.bfloat16),
            jax.ShapeDtypeStruct((3 * places * rows, LANES), jnp.bfloat16),
        ],
        places * rows * LANES * 32,
        *blocks,
    )


def attend(q_ref, kv_refs, state_ref, write, rows, places, room):
    keys_each = kv_refs[0].shape[0] // 3
    jobs = [(i * rows, rows, 0) for i in range(places)] + [(places * rows, places * room, 1)]
    for start, count, audio in jobs:
        factor = AUDIO_FACTOR if audio else VIDEO_FACTOR
        query = q_ref[start : start + count]
        first, second = ((2, 2) if audio else (0, 1))
        keys = jnp.concatenate([r[first * keys_each : (first + 1) * keys_each] for r in kv_refs], axis=0)
        values = jnp.concatenate(
            [r[second * keys_each : (second + 1) * keys_each] for r in kv_refs], axis=0
        )
        scores = dot_t(query, keys)
        newest = jnp.max(scores, axis=1, keepdims=True)
        if state_ref is not None:
            before = state_ref[start : start + count, LANES : LANES + 1]
            newest = jnp.maximum(newest, before)
        weights = jnp.exp2((scores - newest) * factor)
        summed = jnp.sum(weights, axis=1, keepdims=True)
        mixed = dot_n(weights.astype(jnp.bfloat16), values)
        if state_ref is not None:
            shrink = jnp.exp2((before - newest) * factor)
            summed = summed + shrink * state_ref[start : start + count, LANES + 1 : LANES + 2]
            mixed = mixed + shrink * state_ref[start : start + count, :LANES]
        write(start, count, factor, newest, summed, mixed)


def attend_state(queries, blocks, state, rows, places, room):
    given = [] if state is None else [state]

    def kernel(q_ref, *refs):
        kv_refs, o_ref = (refs[: len(blocks)], refs[-1])

        def write(start, count, factor, newest, summed, mixed):
            lane = lane_of(count)
            o_ref[start : start + count, :LANES] = mixed
            o_ref[start : start + count, LANES:] = jnp.where(lane == 0, newest, summed)

        attend(q_ref, kv_refs, refs[len(blocks)] if given else None, write, rows, places, room)

    return kernel_call(
        kernel,
        jax.ShapeDtypeStruct((queries.shape[0], 2 * LANES), jnp.float32),
        4 * queries.shape[0] * len(blocks) * blocks[0].shape[0] // 3 * LANES,
        queries,
        *blocks,
        *given,
    )


def attend_away(queries, blocks, state, rows, places, room, visits):
    def kernel(q_ref, *refs):
        kv_refs, state_ref, o_ref = (refs[: len(blocks)], refs[-2], refs[-1])
        levels = []

        def parts_of(level):
            high = level.astype(jnp.bfloat16).astype(jnp.float32)
            middle = (level - high).astype(jnp.bfloat16).astype(jnp.float32)
            return (high, middle, level - high - middle)

        def write(start, count, factor, newest, summed, mixed):
            level = newest * factor + jnp.log2(summed)
            mixed = mixed / summed
            if start < places * rows:
                levels.append(level)
                o_ref[start : start + count] = mixed.astype(jnp.bfloat16)
                return
            for i in range(places):
                lane = lane_of(visits)
                cut = slice(i * room, i * room + visits)
                tile = jnp.where(lane < AUDIO_DIM, 0.0, mixed[cut])
                columns = [level[cut]]
                columns += [levels[i][k : k + visits] for k in range(0, rows, visits)]
                for k, column in enumerate(columns):
                    for j, part in enumerate(parts_of(column)):
                        tile = jnp.where(lane == 3 * k + j, part, tile)
                tile = jnp.concatenate(
                    (tile, jnp.zeros((room - visits, LANES), jnp.float32)), axis=0
                )
                o_ref[start + i * room : start + (i + 1) * room] = tile.astype(jnp.bfloat16)

        attend(q_ref, kv_refs, state_ref, write, rows, places, room)

    return kernel_call(
        kernel,
        jax.ShapeDtypeStruct(queries.shape, jnp.bfloat16),
        4 * queries.shape[0] * len(blocks) * blocks[0].shape[0] // 3 * LANES,
        queries,
        *blocks,
        state,
    )


def merge(state, back, rows, places, room, visits):
    def kernel(s_ref, b_ref, *o_refs):
        for i in range(places):
            start = places * rows + i * room
            tile = b_ref[start : start + room].astype(jnp.float32)[:visits]

            def level_of(k):
                return sum(tile[:, 3 * k + j : 3 * k + j + 1] for j in range(3))

            video = [level_of(1 + k) for k in range(rows // visits)]
            for at, count, level, factor in (
                (i * rows, rows, jnp.concatenate(video, axis=0), VIDEO_FACTOR),
                (start, visits, level_of(0), AUDIO_FACTOR),
            ):
                other = b_ref[at : at + count] if count == rows else tile
                peak = s_ref[at : at + count, LANES : LANES + 1] * factor
                summed = s_ref[at : at + count, LANES + 1 : LANES + 2]
                newest = jnp.maximum(peak, level)
                here, there = (jnp.exp2(peak - newest), jnp.exp2(level - newest))
                scale = 1.0 / (here * summed + there)
                mixed = s_ref[at : at + count, :LANES] * (here * scale) + other.astype(
                    jnp.float32
                ) * (there * scale)
                if count == rows:
                    o_refs[i][:rows] = mixed.astype(jnp.bfloat16)
                else:
                    mixed = jnp.concatenate(
                        (mixed, jnp.zeros((room - visits, LANES), jnp.float32)), axis=0
                    )
                    o_refs[i][rows:] = mixed.astype(jnp.bfloat16)

    return kernel_call(
        kernel,
        [jax.ShapeDtypeStruct((rows + room, LANES), jnp.bfloat16)] * places,
        state.shape[0] * LANES * 32,
        state,
        back,
    )


def place_heads(arc, parts, rows, visits):
    heads = len(parts)

    def kernel(arc_ref, *refs):
        p_refs, v_ref, a_ref, held = (refs[:heads], refs[heads], refs[heads + 1], refs[heads + 2])
        for i in range(heads):
            held[lax.rem(arc_ref[0] + i, heads)] = p_refs[i][...]
        for h in range(heads):
            v_ref[:, h * LANES : (h + 1) * LANES] = held[h, :rows]
        for g in range(heads // 2):
            low, high = (held[2 * g + i, rows:].astype(jnp.float32)[:visits] for i in range(2))
            low = pltpu.roll(low, AUDIO_DIM, 1)
            both = jnp.where(lane_of(visits) < AUDIO_DIM, low, high)
            a_ref[:, g * LANES : (g + 1) * LANES] = both.astype(jnp.bfloat16)

    return kernel_call(
        kernel,
        [
            jax.ShapeDtypeStruct((rows, heads * LANES), jnp.bfloat16),
            jax.ShapeDtypeStruct((visits, heads * AUDIO_DIM), jnp.bfloat16),
        ],
        rows * heads * LANES * 16,
        arc,
        *parts,
        scalars=1,
        scratch=[pltpu.VMEM((heads,) + parts[0].shape, jnp.bfloat16)],
    )


def one_head(pair, parity):
    lane = lax.broadcasted_iota(jnp.int32, pair.shape, 1)
    keep = (lane < AUDIO_DIM) if parity == 0 else (lane >= AUDIO_DIM)
    return jnp.where(keep, pair, jnp.zeros_like(pair))


def window_attend(queries, near, limits):
    rows, width = queries.shape
    heads = width // AUDIO_DIM
    factor = AUDIO_FACTOR
    span = limits.shape[1] // len(near)
    count = len(near)

    def kernel(q_ref, lim_ref, *refs):
        n_refs, o_ref = (refs[:count], refs[count])
        tile = lax.broadcasted_iota(jnp.int32, (rows, span), 0) // TILE_LEN
        visible = []
        for i in range(count):
            cut = slice(i * span, (i + 1) * span)
            visible.append((lim_ref[0:1, cut] <= tile) & (tile < lim_ref[1:2, cut]))
        lane = lane_of(rows)
        for g in range(heads // 2):
            cols = slice(g * LANES, (g + 1) * LANES)
            pair = q_ref[:, cols]
            mixed = []
            for parity in range(2):
                masked = one_head(pair, parity)
                scores = []
                for i in range(count):
                    keys = n_refs[i][:, cols]
                    scores.append(jnp.where(visible[i], dot_t(masked, keys), jnp.float32(-1e30)))
                newest = jnp.max(scores[0], axis=1, keepdims=True)
                for score in scores[1:]:
                    newest = jnp.maximum(newest, jnp.max(score, axis=1, keepdims=True))
                summed = jnp.zeros((rows, 1), jnp.float32)
                top = jnp.zeros((rows, LANES), jnp.float32)
                for i in range(count):
                    values = n_refs[i][:, width + g * LANES : width + (g + 1) * LANES]
                    weights = jnp.exp2((scores[i] - newest) * factor)
                    summed = summed + jnp.sum(weights, axis=1, keepdims=True)
                    top = top + dot_n(weights.astype(jnp.bfloat16), values)
                mixed.append(top / summed)
            both = jnp.where(lane < AUDIO_DIM, mixed[0], mixed[1])
            o_ref[:, cols] = both.astype(jnp.bfloat16)

    return kernel_call(
        kernel,
        jax.ShapeDtypeStruct((rows, width), jnp.bfloat16),
        4 * rows * span * count * width,
        queries,
        limits,
        *near,
    )


def body(vid_q, vid_k, vid_v, aud_q, cross_k, cross_v, cross_q, aud_k, aud_v, windows):
    n = lax.axis_size("seq")
    places = vid_q.shape[1] // HEAD_DIM
    quad = n // places
    if quad != 4 or n % places != 0 or places % 2 != 0 or lax.axis_size("sub") != 2:
        raise ValueError("mesh shape")

    def swap(array):
        return lax.ppermute(array, "sub", [(0, 1), (1, 0)])

    def shift(array, by):
        return lax.ppermute(array, "seq", [(z, (z + by) % n) for z in range(n)])

    def cross(array, bit):
        return lax.ppermute(array, "seq", [(z, z ^ bit) for z in range(n)])

    def outward(array):
        pairs = []
        for z in range(n):
            right, left = (2 * z + 1, 2 * ((z + 1) % n))
            pairs += [(right, left), (left, right)]
        return lax.ppermute(array, ("seq", "sub"), pairs)

    rows, visits = (vid_q.shape[0], aud_q.shape[0])
    room = padded(visits)
    place = lax.axis_index("seq")
    arc = (place // quad).reshape(1).astype(jnp.int32)

    blocks = pack_heads(arc, vid_q, vid_k, vid_v, aud_q, cross_k, cross_v)
    blocks = [blocks[0]] + [shift(blocks[i], i * quad) for i in range(1, places)]
    queries, own = regroup(blocks, rows, room)

    near = cross(own, 1)
    guests = cross(queries, 2)
    sibling = swap(own)
    near_sibling = swap(near)
    sizes = (rows, places, room)
    guest_state = attend_state(guests, [own, sibling], None, *sizes)
    state = attend_state(queries, [own, sibling], None, *sizes)
    away = attend_away(guests, [near, near_sibling], guest_state, *sizes, visits)
    back = cross(away, 2)
    state = attend_state(queries, [near, near_sibling], state, *sizes)
    parts = merge(state, back, *sizes, visits)
    parts = [parts[0]] + [shift(parts[i], -i * quad) for i in range(1, places)]
    video_self, audio_out = place_heads(arc, parts, rows, visits)

    audio_own = jnp.concatenate((aud_k, aud_v), axis=1)
    position = lax.axis_index(("seq", "sub"))
    stretches = visits // STRETCH_LEN
    tiles = rows // TILE_LEN
    side = 2 * lax.axis_index("sub") - 1
    held = jnp.pad(windows, ((0, 0), (stretches, stretches)))
    limits = jnp.concatenate(
        [
            lax.dynamic_slice_in_dim(held, (position + d + 1) * stretches, stretches, axis=1)
            for d in (0, side, -side)
        ],
        axis=1,
    )
    limits = jnp.repeat(limits - position * tiles, STRETCH_LEN, axis=1)
    video_cross = window_attend(
        cross_q, [audio_own, outward(audio_own), swap(audio_own)], limits
    )
    return (video_self, audio_out, video_cross)


def solution(mesh):
    rows = P(("grp", "seq", "sub"), "head")
    return jax.shard_map(
        body,
        mesh=mesh,
        in_specs=(rows,) * 9 + (P(None, "grp"),),
        out_specs=(rows, rows, rows),
        check_vma=False,
    )
```
